32 devices in a mesh: seq: 8 (over z, y), rep: 4 (over x, core).
Axes of the slice: x: 2, y: 2, z: 4, core: 2. Of those that a mesh axis runs over, the one named last changes fastest.
Arguments:
- inputs: bfloat16 [4, 1024, 1024], P('rep', 'seq'), may hold values from -6 to 6
- weight_t: bfloat16 [3072, 1024], P('seq', 'rep'), may hold values from -0.1875 to 0.1875
- states: float32 [4, 1024, 1024], P('rep', 'seq'), may hold values from -0.9 to 0.9
- doc_ids: int32 [4, 1024], P('rep', 'seq'), may hold values from 0 to 3, never falling along the last dimension, each value on 1 to 512 neighbouring positions
- recur: float32 [3, 1024], replicated, may hold values from -1 to 1
- bias: float32 [3, 1024], replicated, may hold values from -8 to 3, as said below
- out_grad: bfloat16 [4, 1024, 1024], P('rep', 'seq'), may hold values from -6 to 6
Outputs:
- input_grad: bfloat16 [4, 1024, 1024], P('rep', 'seq')
- weight_grad: float32 [3072, 1024], P('seq', 'rep')
- param_grad: float32 [6, 1024], replicated
The draws below stay inside these ranges and needn't reach their ends.
Inputs may be any that keep to these rules, and one draw needn't show every extreme that they name: `doc_ids`: within each sequence the numbers never fall; every document has 1 to 512 tokens, and some document has exactly 512. `bias`: row 0 lies between -8 and -1, rows 1 and 2 between -3 and 3.
All inputs are finite; a program needn't handle non-finite values.
Results may differ from the reference program's by a relative error of at most 0.0095.
Values may be sent and summed in bfloat16 or wider, within the bound.
A program may use at most 128 MiB of HBM per device.

```python
import math
import jax
import jax.numpy as jnp
import numpy as np
from jax import lax

DI = 1024
H = 1024
L = 1024
SEQS = 4
SEGS = 4
MOST = 512


def draw_bias(key, part):
    keys = jax.random.split(jax.random.fold_in(key, 17), 4)
    share = 0.5
    others = jnp.clip(jax.random.normal(keys[3], (2, H), jnp.float32), -3.0, 3.0)
    slower = jax.random.uniform(keys[0], (H,), jnp.float32) < share
    slow_value = jax.random.uniform(keys[1], (H,), jnp.float32, -8.0, -6.0)
    fast_value = jax.random.uniform(keys[2], (H,), jnp.float32, -3.0, -1.0)
    first = jnp.where(slower, slow_value, fast_value)
    return jnp.concatenate([first[None, :], others], 0).astype(jnp.float32)


def block_levels(rng, extent, cuts, least, high):
    level = 1.0
    for position, blocks in cuts:
        draws = jax.random.uniform(jax.random.fold_in(jax.random.fold_in(rng, 6), position), (blocks,), jnp.float32, least / len(cuts), high / len(cuts))
        level = level * jnp.repeat(jnp.exp(draws), extent[position] // blocks).reshape((-1,) + (1,) * (len(extent) - 1 - position))
    return level


def profile(amount, total, reach, slope):
    loads = [(1 << 20) // math.isqrt(standing ** slope) + 1 for standing in range(2, amount + 1)]
    spare, counts = total - reach - (amount - 1), [1] * (amount - 1)
    while spare > 0:
        candidates = [i for i in range(amount - 1) if counts[i] < reach]
        pool, budget = sum([loads[i] for i in candidates]), spare
        for i in candidates:
            addition = min(reach - counts[i], max(1, budget * loads[i] // pool), spare)
            counts[i] = counts[i] + addition
            spare = spare - addition
    return np.array([reach] + counts)


def uneven(stream_key, count, total, most, lean):
    if count == 2:
        one = jax.random.randint(stream_key, (), max(1, total - most), min(most, total - 1) + 1)
        return jnp.stack([one, total - one])
    sizes = jnp.asarray(profile(count, total, most, lean), jnp.int32)
    couples = (count - 1) // 2
    giver, receiver = sizes[1:1 + 2 * couples:2], sizes[2:2 + 2 * couples:2]
    room = jnp.minimum(giver - 1, most - receiver)
    moved = jax.random.randint(jax.random.fold_in(stream_key, 1), (couples,), 0, 1 << 20) % (room + 1)
    sizes = sizes.at[1:1 + 2 * couples:2].set(giver - moved).at[2:2 + 2 * couples:2].set(receiver + moved)
    return sizes[jax.random.permutation(jax.random.fold_in(stream_key, 2), count)]


def bell_draw(rng, extent, scale, limit, shards=(), kind=jnp.bfloat16):
    array = scale * jax.random.normal(rng, extent, jnp.float32)
    if shards:
        array = array * block_levels(rng, extent, shards, -0.22, 0.18)
    return jnp.clip(array, -limit, limit).astype(kind)


def setup_inputs(seed: int = 0) -> dict:
    key_of = jax.random.split(jax.random.key(seed), 8)
    return {
        "inputs": bell_draw(key_of[0], (SEQS, L, DI), 1.0, 6.0, ((0, 4), (1, 8))),
        "weight_t": bell_draw(key_of[1], (3 * H, DI), DI ** -0.5, 0.1875, ((0, 8), (1, 4))),
        "states": jnp.clip(jax.random.uniform(key_of[2], (SEQS, L, H), jnp.float32, -0.9, 0.9) * block_levels(key_of[2], (SEQS, L, H), ((0, 4), (1, 8)), -0.4, 0.0), -0.9, 0.9),
        "doc_ids": jax.vmap(lambda own: jnp.searchsorted(jnp.cumsum(uneven(own, SEGS, L, MOST, 1)), jnp.arange(L), side="right"))(jax.random.split(key_of[3], SEQS)).reshape((SEQS, L)).astype(jnp.int32),
        "recur": jnp.clip(jax.random.uniform(key_of[4], (3, H), jnp.float32, -1.0, 1.0), -1.0, 1.0),
        "bias": draw_bias(jax.random.fold_in(key_of[7], 71), 0),
        "out_grad": bell_draw(key_of[6], (SEQS, L, H), 1.0, 6.0, ((0, 4), (1, 8))),
    }


def one_sequence(feats, states, doc_ids, out_grad, weight_t, recur, bias):
    preact = jnp.dot(feats, weight_t.T, preferred_element_type=jnp.float32)
    pz = preact[:, :H]
    pr = preact[:, H:2 * H]
    pc = preact[:, 2 * H:]
    same = jnp.concatenate([jnp.zeros((1,), jnp.float32), (doc_ids[1:] == doc_ids[:-1]).astype(jnp.float32)])
    prior = jnp.concatenate([jnp.zeros((1, H), jnp.float32), states[:-1]], 0) * same[:, None]
    gate_z = jax.nn.sigmoid(pz + recur[0] * prior + bias[0])
    gate_r = jax.nn.sigmoid(pr + recur[1] * prior + bias[1])
    gate_c = jnp.tanh(pc + recur[2] * gate_r * prior + bias[2])
    jacobian = same[:, None] * (1.0 - gate_z + (gate_c - prior) * gate_z * (1.0 - gate_z) * recur[0] + gate_z * (1.0 - gate_c * gate_c) * recur[2] * (gate_r + prior * gate_r * (1.0 - gate_r) * recur[1]))
    factor = jnp.concatenate([jacobian[1:], jnp.zeros((1, H), jnp.float32)], 0)

    def backstep(carry, item):
        upstream, coef = item
        adjoint = upstream + coef * carry
        return (adjoint, adjoint)
    _, adjoint = lax.scan(backstep, jnp.zeros((H,), jnp.float32), (out_grad.astype(jnp.float32), factor), reverse=True)
    grad_z = adjoint * (gate_c - prior) * gate_z * (1.0 - gate_z)
    grad_c = adjoint * gate_z * (1.0 - gate_c * gate_c)
    grad_r = grad_c * recur[2] * prior * gate_r * (1.0 - gate_r)
    grad_pre = jnp.concatenate([grad_z, grad_r, grad_c], 1).astype(jnp.bfloat16)
    input_grad = jnp.dot(grad_pre, weight_t, preferred_element_type=jnp.float32).astype(jnp.bfloat16)
    weight_part = jnp.dot(grad_pre.T, feats, preferred_element_type=jnp.float32)
    stats = jnp.stack([grad_z.sum(0), grad_r.sum(0), grad_c.sum(0), (grad_z * prior).sum(0), (grad_r * prior).sum(0), (grad_c * gate_r * prior).sum(0)])
    return (input_grad, weight_part, stats)

def reference(inputs, weight_t, states, doc_ids, recur, bias, out_grad):

    def single(items):
        return one_sequence(items[0], items[1], items[2], items[3], weight_t, recur, bias)
    input_grad, weight_parts, stats = lax.map(single, (inputs, states, doc_ids, out_grad))
    factor = 1.0 / math.sqrt(SEQS * L)
    return (input_grad, weight_parts.sum(0) * factor, stats.sum(0) * factor)
```

```python
import functools
import math

import jax
import jax.numpy as jnp
from jax import lax
from jax.experimental import pallas as pl
from jax.experimental.pallas import tpu as pltpu
from jax.sharding import PartitionSpec as P

F32 = jnp.float32
BF16 = jnp.bfloat16
GATES = 3


def shifted(block, axis, distance):
    devices = range(lax.axis_size(axis))
    route = [(i - distance, i) for i in devices if i - distance in devices]
    return lax.ppermute(block, axis, route)


def compose(earlier, later):
    return (later[0] * earlier[0], later[1] + later[0] * earlier[1])


def by_tokens(inputs, weight_t, states, doc_ids, recur, bias, out_grad):
    feats = inputs[0]
    hidden_now = states[0]
    ids_float = doc_ids[0].astype(F32)
    count = feats.shape[0]
    width = hidden_now.shape[1]
    columns = lax.all_gather(weight_t, "rep", axis=1, tiled=True)
    contract_last = (((1,), (1,)), ((), ()))
    full_weight = lax.all_gather(columns, "seq", axis=0, tiled=True)
    preact = lax.dot_general(feats, full_weight, contract_last, preferred_element_type=F32)
    tail_state, tail_id = shifted((hidden_now[-1:], ids_float[-1:]), "seq", 1)
    first_same = jnp.where(
        (ids_float[0] == tail_id[0]) & (lax.axis_index("seq") > 0), 1.0, 0.0
    ).astype(F32)
    same = jnp.concatenate([first_same[None], (ids_float[1:] == ids_float[:-1]).astype(F32)])
    prior = jnp.concatenate([tail_state, hidden_now[:-1]], 0) * same[:, None]
    gate_z = jax.nn.sigmoid(preact[:, :width] + recur[0] * prior + bias[0])
    gate_r = jax.nn.sigmoid(preact[:, width : 2 * width] + recur[1] * prior + bias[1])
    gate_c = jnp.tanh(preact[:, 2 * width :] + recur[2] * gate_r * prior + bias[2])
    jacobian = same[:, None] * (
        1.0
        - gate_z
        + (gate_c - prior) * gate_z * (1.0 - gate_z) * recur[0]
        + gate_z
        * (1.0 - gate_c * gate_c)
        * recur[2]
        * (gate_r + prior * gate_r * (1.0 - gate_r) * recur[1])
    )
    upstream = out_grad[0].astype(F32)
    jac_rows, up_rows = (
        lax.all_to_all(jacobian.T, "seq", split_axis=0, concat_axis=1, tiled=True),
        lax.all_to_all(upstream.T, "seq", split_axis=0, concat_axis=1, tiled=True),
    )
    factor = jnp.concatenate([jac_rows[:, 1:], jnp.zeros((jac_rows.shape[0], 1), F32)], 1)
    _, adjoint_rows = lax.associative_scan(compose, (factor, up_rows), reverse=True, axis=1)
    adjoint = lax.all_to_all(adjoint_rows, "seq", split_axis=1, concat_axis=0, tiled=True).T
    grad_z = adjoint * (gate_c - prior) * gate_z * (1.0 - gate_z)
    grad_c = adjoint * gate_z * (1.0 - gate_c * gate_c)
    grad_r = grad_c * recur[2] * prior * gate_r * (1.0 - gate_r)
    grad_pre = jnp.concatenate([grad_z, grad_r, grad_c], 1).astype(BF16)
    input_grad = jnp.dot(grad_pre, full_weight, preferred_element_type=F32)
    tokens_all = count * inputs.shape[0] * lax.axis_size("seq") * lax.axis_size("rep")
    normal_factor = 1.0 / math.sqrt(tokens_all)
    row_share = lax.psum_scatter(
        lax.dot_general(grad_pre, feats, (((0,), (0,)), ((), ())), preferred_element_type=F32),
        "seq",
        scatter_dimension=0,
        tiled=True,
    )
    weight_grad = (
        lax.psum_scatter(row_share.astype(BF16), "rep", scatter_dimension=1, tiled=True).astype(F32)
        * normal_factor
    )
    stats = jnp.stack(
        [
            grad_z.sum(0),
            grad_r.sum(0),
            grad_c.sum(0),
            (grad_z * prior).sum(0),
            (grad_r * prior).sum(0),
            (grad_c * gate_r * prior).sum(0),
        ]
    )
    param_grad = lax.psum(stats, ("seq", "rep")) * normal_factor
    return (input_grad.astype(BF16)[None], weight_grad, param_grad)


def swap_roles(a, b):
    return 2 * (a // 2) + b % 2, 2 * (b // 2) + a % 2


def kernel(
    ns, nr, feats, weight, states, ids, recur, bias, upstream,
    out_in, out_w, out_p,
    pay_src, pay, ids_src, ids_all, x_all, w_all, prev, ids_col, up, jac, co_z, co_r, co_c, rprior,
    scan_a, scan_b, carry, lam, grads, part_out, part_in, part_keep, fin_out, fin_in, wg_out, wg_in,
    st_out, st_in,
    x_s0, x_sz, x_sd, x_r, w_s1, w_s2, w_r, p_s, p_r, i_s, i_r, d_s, d_r, f_s, f_r, g_s, g_r, t_s, t_r,
):
    T, DI = feats.shape
    H = states.shape[1]
    hb, cw, nz = H // ns, DI // nr, ns // 2
    s, r = lax.axis_index("seq"), lax.axis_index("rep")
    k, q = swap_roles(s, r)
    z, c = k // 2, k % 2
    me = s * nr + r
    unsent = []

    def place(a, b):
        return {"seq": a, "rep": b}

    def send(src, dst, ssem, rsem, where):
        pltpu.make_async_remote_copy(
            src_ref=src, dst_ref=dst, send_sem=ssem, recv_sem=rsem,
            device_id=where, device_id_type=pl.DeviceIdType.MESH,
        ).start()

    def local(src, dst, rsem):
        pltpu.make_async_copy(src, dst, rsem).start()

    def landed(dst, sem):
        pltpu.make_async_copy(dst, dst, sem).wait()

    def send_or_local(src, dst, ssem, rsem, where, here):
        @pl.when(jnp.logical_not(here))
        def _():
            send(src, dst, ssem, rsem, place(*where))

        @pl.when(here)
        def _():
            local(src, dst, rsem)

        unsent.append((jnp.logical_not(here), src, ssem))

    def rows(ref, block, count):
        return ref.at[pl.ds(pl.multiple_of(block * count, count), count), :]

    for j in range(ns):
        pay_src[j, :, :hb] = states[:, j * hb : (j + 1) * hb].astype(BF16)
        pay_src[j, :, hb:] = upstream[:, j * hb : (j + 1) * hb]
    ids_src[...] = jnp.broadcast_to(ids[...].astype(F32), ids_src.shape)

    barrier = pltpu.get_barrier_semaphore()

    def greet(d, _):
        @pl.when(d != me)
        def _():
            pl.semaphore_signal(
                barrier, inc=1, device_id=place(d // nr, d % nr), device_id_type=pl.DeviceIdType.MESH
            )

        return 0

    lax.fori_loop(0, ns * nr, greet, 0)
    pl.semaphore_wait(barrier, ns * nr - 1)

    diagonal = (s % 2) == (r % 2)
    send_or_local(feats, rows(x_all, s, T), x_s0, x_r.at[s], swap_roles(s, r), diagonal)
    for i in range(GATES):
        b = GATES * s + i
        g, j = b // ns, b % ns
        dst = w_all.at[
            pl.ds(pl.multiple_of(g * hb, hb), hb), pl.ds(pl.multiple_of(r * cw, cw), cw)
        ]
        send_or_local(
            weight.at[i * hb : (i + 1) * hb, :], dst, w_s1.at[i], w_r.at[g * nr + r],
            (2 * (j // 2) + s % 2, 2 * (r // 2) + j % 2), j == k,
        )
    for j in range(ns):
        here = jnp.logical_and(diagonal, k == j)
        where = swap_roles(j, r)
        send_or_local(ids_src, ids_all.at[s], i_s.at[j], i_r.at[s], where, here)
        send_or_local(pay_src.at[j], pay.at[s], p_s.at[j], p_r.at[s], where, here)

    mine = rows(x_all, k, T)
    landed(mine, x_r.at[k])
    for other in range(nz):
        away = other != z

        @pl.when(away)
        def _():
            send(mine, mine, x_sz.at[other], x_r.at[k], place(*swap_roles(2 * other + c, q)))

        unsent.append((away, mine, x_sz.at[other]))
    partner = place(*swap_roles(k + 1 - 2 * c, q))
    send(mine, mine, x_sd.at[z], x_r.at[k], partner)

    def weight_slot(g, col):
        return w_all.at[g * hb : (g + 1) * hb, col * cw : (col + 1) * cw]

    relays = {}
    for g in range(GATES):
        for col in range(nr):
            relay = jnp.logical_and(((g * ns + k) // GATES) % 2 == s % 2, r // 2 == col // 2)
            relays[g, col] = relay
            slot = weight_slot(g, col)

            @pl.when(relay)
            def _():
                landed(slot, w_r.at[g * nr + col])

            for other in range(nr):
                away = jnp.logical_and(relay, q != other)
                sem = w_s2.at[(g * nr + col) * nr + other]

                @pl.when(away)
                def _():
                    send(slot, slot, sem, w_r.at[g * nr + col], place(*swap_roles(k, other)))

                unsent.append((away, slot, sem))

    for other in range(nz):
        block = 2 * other + c
        there = rows(x_all, block, T)

        @pl.when(other != z)
        def _():
            landed(there, x_r.at[block])
            send(there, there, x_sd.at[other], x_r.at[block], partner)

        unsent.append((None, there, x_sd.at[other]))

    prev[0:8, :] = jnp.zeros((8, hb), F32)
    ids_col[0:8, :] = jnp.full((8, hb), -1.0, F32)
    jac[ns * T : ns * T + 8, :] = jnp.zeros((8, hb), F32)
    for m in range(ns):
        landed(ids_all.at[m], i_r.at[m])
        landed(pay.at[m], p_r.at[m])
        prev[8 + m * T : 8 + (m + 1) * T, :] = pay[m, :, :hb].astype(F32)
        up[m * T : (m + 1) * T, :] = pay[m, :, hb:].astype(F32)
        ids_col[8 + m * T : 8 + (m + 1) * T, :] = jnp.broadcast_to(ids_all[m, 0:1, :], (hb, T)).T

    for other in range(nz):
        block = 2 * other + 1 - c
        landed(rows(x_all, block, T), x_r.at[block])
    for g in range(GATES):
        for col in range(nr):

            @pl.when(jnp.logical_not(relays[g, col]))
            def _():
                landed(weight_slot(g, col), w_r.at[g * nr + col])

    group = pl.ds(pl.multiple_of(k * hb, hb), hb)
    rz, rr, rc = (recur[i : i + 1, group] for i in range(GATES))
    bz, br, bc = (bias[i : i + 1, group] for i in range(GATES))
    for m in range(ns):
        span = slice(m * T, (m + 1) * T)
        pre = lax.dot_general(
            x_all[span, :], w_all[...], (((1,), (1,)), ((), ())), preferred_element_type=F32
        )
        same = jnp.where(
            ids_col[8 + m * T : 8 + (m + 1) * T, :] == ids_col[7 + m * T : 7 + (m + 1) * T, :], 1.0, 0.0
        )
        prior = prev[7 + m * T : 7 + (m + 1) * T, :] * same
        gz = jax.nn.sigmoid(pre[:, :hb] + rz * prior + bz)
        gr = jax.nn.sigmoid(pre[:, hb : 2 * hb] + rr * prior + br)
        rp = gr * prior
        gc = jnp.tanh(pre[:, 2 * hb :] + rc * rp + bc)
        az = (gc - prior) * gz * (1.0 - gz)
        ac = gz * (1.0 - gc * gc)
        slope = rp * (1.0 - gr)
        acr = ac * rc
        co_z[span, :] = az
        co_c[span, :] = ac
        co_r[span, :] = acr * slope
        rprior[span, :] = rp
        jac[span, :] = same * (1.0 - gz + az * rz + acr * (gr + slope * rr))

    def back(i, state):
        a, b = state
        t = T - 1 - i
        f = jac[pl.ds(t + 1, ns, stride=T), :]
        u = up[pl.ds(t, ns, stride=T), :]
        a, b = f * a, u + f * b
        scan_a[t] = a
        scan_b[t] = b
        return a, b

    a, b = lax.fori_loop(0, T, back, (jnp.ones((ns, hb), F32), jnp.zeros((ns, hb), F32)), unroll=8)
    tail = jnp.zeros((1, hb), F32)
    for m in reversed(range(ns)):
        carry[m : m + 1, :] = tail
        tail = b[m : m + 1, :] + a[m : m + 1, :] * tail
    carried = carry[...]

    def finish(t, _):
        lam[pl.ds(t, ns, stride=T), :] = scan_b[t] + scan_a[t] * carried
        return 0

    lax.fori_loop(0, T, finish, 0, unroll=8)

    sums = [jnp.zeros((1, hb), F32) for _ in range(6)]
    for m in range(ns):
        span = slice(m * T, (m + 1) * T)
        same = jnp.where(
            ids_col[8 + m * T : 8 + (m + 1) * T, :] == ids_col[7 + m * T : 7 + (m + 1) * T, :], 1.0, 0.0
        )
        prior = prev[7 + m * T : 7 + (m + 1) * T, :] * same
        adj = lam[span, :]
        grad_z = adj * co_z[span, :]
        grad_r = adj * co_r[span, :]
        grad_c = adj * co_c[span, :]
        grads[span, :hb] = grad_z.astype(BF16)
        grads[span, hb : 2 * hb] = grad_r.astype(BF16)
        grads[span, 2 * hb :] = grad_c.astype(BF16)
        terms = (grad_z, grad_r, grad_c, grad_z * prior, grad_r * prior, grad_c * rprior[span, :])
        sums = [total + jnp.sum(term, 0, keepdims=True) for total, term in zip(sums, terms)]
    for i in range(6):
        st_out[i : i + 1, :] = sums[i]
    st_out[6:8, :] = jnp.zeros((2, hb), F32)

    for other in range(nz):
        block = 2 * other + 1 - c
        part_out[other] = jnp.dot(
            rows(grads, block, T)[...], w_all[...], preferred_element_type=F32
        ).astype(BF16)
        send(part_out.at[other], part_in.at[other], d_s.at[other], d_r.at[other], partner)
        unsent.append((None, part_out.at[other], d_s.at[other]))
    for other in range(nz):
        part_keep[other] = jnp.dot(
            rows(grads, 2 * other + c, T)[...], w_all[...], preferred_element_type=F32
        )

    for other in range(nz):
        landed(part_in.at[other], d_r.at[other])
        fin_out[other] = (part_keep[other] + part_in[other].astype(F32)).astype(BF16)
        block = 2 * other + c
        here = jnp.logical_and(block == s, q == r)
        send_or_local(fin_out.at[other], fin_in.at[z], f_s.at[other], f_r.at[z], (block, q), here)

    slot = k * nr + q
    st_in[slot] = st_out[...]

    def tell(d, _):
        @pl.when(d != me)
        def _():
            send(st_out, st_in.at[slot], t_s.at[d], t_r.at[slot], place(d // nr, d % nr))

        return 0

    lax.fori_loop(0, ns * nr, tell, 0)

    for g in range(GATES):
        wg_out[g] = lax.dot_general(
            grads[:, g * hb : (g + 1) * hb], x_all[...], (((0,), (0,)), ((), ())),
            preferred_element_type=F32,
        ).astype(BF16)
        b = g * ns + k
        owner, i = b // GATES, b % GATES
        for col in range(nr):
            here = jnp.logical_and(owner == s, r == col)
            send_or_local(
                wg_out.at[g, :, col * cw : (col + 1) * cw], wg_in.at[q * GATES + i],
                g_s.at[g * nr + col], g_r.at[q * GATES + i], (owner, col), here,
            )

    scale = 1.0 / math.sqrt(ns * nr * T)
    total = None
    for other in range(nz):
        landed(fin_in.at[other], f_r.at[other])
        term = fin_in[other].astype(F32)
        total = term if total is None else total + term
    out_in[...] = total.astype(BF16)

    def heard(d, _):
        @pl.when(d != slot)
        def _():
            landed(st_in.at[d], t_r.at[d])

        return 0

    lax.fori_loop(0, ns * nr, heard, 0)
    for j in range(ns):
        total = st_in[j * nr]
        for other in range(1, nr):
            total = total + st_in[j * nr + other]
        out_p[:, j * hb : (j + 1) * hb] = total[:6] * scale

    for i in range(GATES):
        total = None
        for other in range(nr):
            landed(wg_in.at[other * GATES + i], g_r.at[other * GATES + i])
            term = wg_in[other * GATES + i].astype(F32)
            total = term if total is None else total + term
        out_w[i * hb : (i + 1) * hb, :] = total * scale

    def told(d, _):
        @pl.when(d != me)
        def _():
            landed(st_out, t_s.at[d])

        return 0

    lax.fori_loop(0, ns * nr, told, 0)
    for sent, src, sem in unsent:
        if sent is None:
            landed(src, sem)
        else:

            @pl.when(sent)
            def _():
                landed(src, sem)


def by_hidden(ns, nr, inputs, weight_t, states, doc_ids, recur, bias, out_grad):
    T, DI = inputs.shape[1:]
    H = states.shape[2]
    hb, cw, nz = H // ns, DI // nr, ns // 2
    L = ns * T
    vm = pltpu.VMEM
    scratch = [
        vm((ns, T, 2 * hb), BF16),
        vm((ns, T, 2 * hb), BF16),
        vm((8, T), F32),
        vm((ns, 8, T), F32),
        vm((L, DI), BF16),
        vm((GATES * hb, DI), BF16),
        vm((L + 8, hb), F32),
        vm((L + 8, hb), F32),
        vm((L, hb), F32),
        vm((L + 8, hb), F32),
        vm((L, hb), F32),
        vm((L, hb), F32),
        vm((L, hb), F32),
        vm((L, hb), F32),
        vm((T, ns, hb), F32),
        vm((T, ns, hb), F32),
        vm((ns, hb), F32),
        vm((L, hb), F32),
        vm((L, GATES * hb), BF16),
        vm((nz, T, DI), BF16),
        vm((nz, T, DI), BF16),
        vm((nz, T, DI), F32),
        vm((nz, T, DI), BF16),
        vm((nz, T, DI), BF16),
        vm((GATES, hb, DI), BF16),
        vm((nr * GATES, hb, cw), BF16),
        vm((8, hb), F32),
        vm((ns * nr, 8, hb), F32),
    ]
    dma = pltpu.SemaphoreType.DMA
    counts = [
        None, nz, nz, ns, GATES, GATES * nr * nr, GATES * nr, ns, ns, ns, ns, nz, nz, nz, nz,
        GATES * nr, GATES * nr, ns * nr, ns * nr,
    ]
    sems = [dma if n is None else dma((n,)) for n in counts]
    whole = pl.BlockSpec(memory_space=pltpu.VMEM)
    out_in, out_w, out_p = pl.pallas_call(
        functools.partial(kernel, ns, nr),
        out_shape=(
            jax.ShapeDtypeStruct((T, DI), BF16),
            jax.ShapeDtypeStruct(weight_t.shape, F32),
            jax.ShapeDtypeStruct((6, H), F32),
        ),
        in_specs=[whole] * 7,
        out_specs=(whole,) * 3,
        scratch_shapes=scratch + sems,
        compiler_params=pltpu.CompilerParams(
            collective_id=0, has_side_effects=True, vmem_limit_bytes=56 * 1024 * 1024
        ),
    )(inputs[0], weight_t, states[0], doc_ids, recur, bias, out_grad[0])
    return out_in[None], out_w, out_p


def fits(ns, nr, inputs, weight_t, states):
    parts, L, DI = inputs.shape
    H = states.shape[2]
    return (
        parts == nr
        and ns % 8 == 0
        and nr % 2 == 0
        and H % (ns * 128) == 0
        and DI % (nr * 128) == 0
        and L % (ns * 128) == 0
        and L * DI <= 1 << 21
    )


def solution(mesh):
    ns, nr = mesh.shape["seq"], mesh.shape["rep"]
    placed = (
        P("rep", "seq", None),
        P("seq", "rep"),
        P("rep", "seq", None),
        P("rep", "seq"),
        P(),
        P(),
        P("rep", "seq", None),
    )

    def run(inputs, weight_t, states, doc_ids, recur, bias, out_grad):
        kernelized = fits(ns, nr, inputs, weight_t, states)
        body = functools.partial(by_hidden, ns, nr) if kernelized else by_tokens
        return jax.shard_map(
            body,
            mesh=mesh,
            in_specs=placed,
            out_specs=(P("rep", "seq", None), P("seq", "rep"), P()),
            check_vma=False,
        )(inputs, weight_t, states, doc_ids, recur, bias, out_grad)

    return run
```

```python
import functools
import math

import jax
import jax.numpy as jnp
from jax import lax
from jax.experimental import pallas as pl
from jax.experimental.pallas import tpu as pltpu
from jax.sharding import PartitionSpec as P

F32 = jnp.float32
BF16 = jnp.bfloat16
GATES = 3


def shifted(block, axis, distance):
    devices = range(lax.axis_size(axis))
    route = [(i - distance, i) for i in devices if i - distance in devices]
    return lax.ppermute(block, axis, route)


def compose(earlier, later):
    return (later[0] * earlier[0], later[1] + later[0] * earlier[1])


def by_tokens(inputs, weight_t, states, doc_ids, recur, bias, out_grad):
    feats = inputs[0]
    hidden_now = states[0]
    ids_float = doc_ids[0].astype(F32)
    count = feats.shape[0]
    width = hidden_now.shape[1]
    columns = lax.all_gather(weight_t, "rep", axis=1, tiled=True)
    contract_last = (((1,), (1,)), ((), ()))
    full_weight = lax.all_gather(columns, "seq", axis=0, tiled=True)
    preact = lax.dot_general(feats, full_weight, contract_last, preferred_element_type=F32)
    tail_state, tail_id = shifted((hidden_now[-1:], ids_float[-1:]), "seq", 1)
    first_same = jnp.where(
        (ids_float[0] == tail_id[0]) & (lax.axis_index("seq") > 0), 1.0, 0.0
    ).astype(F32)
    same = jnp.concatenate([first_same[None], (ids_float[1:] == ids_float[:-1]).astype(F32)])
    prior = jnp.concatenate([tail_state, hidden_now[:-1]], 0) * same[:, None]
    gate_z = jax.nn.sigmoid(preact[:, :width] + recur[0] * prior + bias[0])
    gate_r = jax.nn.sigmoid(preact[:, width : 2 * width] + recur[1] * prior + bias[1])
    gate_c = jnp.tanh(preact[:, 2 * width :] + recur[2] * gate_r * prior + bias[2])
    jacobian = same[:, None] * (
        1.0
        - gate_z
        + (gate_c - prior) * gate_z * (1.0 - gate_z) * recur[0]
        + gate_z
        * (1.0 - gate_c * gate_c)
        * recur[2]
        * (gate_r + prior * gate_r * (1.0 - gate_r) * recur[1])
    )
    upstream = out_grad[0].astype(F32)
    jac_rows, up_rows = (
        lax.all_to_all(jacobian.T, "seq", split_axis=0, concat_axis=1, tiled=True),
        lax.all_to_all(upstream.T, "seq", split_axis=0, concat_axis=1, tiled=True),
    )
    factor = jnp.concatenate([jac_rows[:, 1:], jnp.zeros((jac_rows.shape[0], 1), F32)], 1)
    _, adjoint_rows = lax.associative_scan(compose, (factor, up_rows), reverse=True, axis=1)
    adjoint = lax.all_to_all(adjoint_rows, "seq", split_axis=1, concat_axis=0, tiled=True).T
    grad_z = adjoint * (gate_c - prior) * gate_z * (1.0 - gate_z)
    grad_c = adjoint * gate_z * (1.0 - gate_c * gate_c)
    grad_r = grad_c * recur[2] * prior * gate_r * (1.0 - gate_r)
    grad_pre = jnp.concatenate([grad_z, grad_r, grad_c], 1).astype(BF16)
    input_grad = jnp.dot(grad_pre, full_weight, preferred_element_type=F32)
    tokens_all = count * inputs.shape[0] * lax.axis_size("seq") * lax.axis_size("rep")
    normal_factor = 1.0 / math.sqrt(tokens_all)
    row_share = lax.psum_scatter(
        lax.dot_general(grad_pre, feats, (((0,), (0,)), ((), ())), preferred_element_type=F32),
        "seq",
        scatter_dimension=0,
        tiled=True,
    )
    weight_grad = (
        lax.psum_scatter(row_share.astype(BF16), "rep", scatter_dimension=1, tiled=True).astype(F32)
        * normal_factor
    )
    stats = jnp.stack(
        [
            grad_z.sum(0),
            grad_r.sum(0),
            grad_c.sum(0),
            (grad_z * prior).sum(0),
            (grad_r * prior).sum(0),
            (grad_c * gate_r * prior).sum(0),
        ]
    )
    param_grad = lax.psum(stats, ("seq", "rep")) * normal_factor
    return (input_grad.astype(BF16)[None], weight_grad, param_grad)


def kernel(
    ns, nr, feats, weight, states, ids, recur, bias, upstream,
    out_in, out_w, out_p,
    pay_src, pay, ids_src, ids_all, tail_src, tail_in, x_all, w_all, prev, ids_col, up, jac,
    co_z, co_r, co_c, rprior, prior_all,
    scan_a, scan_b, carry, seg_out, seg_in, lam, grads, part_out, part_in, part_keep, fin_out, fin_in,
    wg_out, wg_in, st_out, st_in,
    x_s0, x_sx, x_sy, x_sd, x_r, w_s, w_r, p_s, p_r, i_s, i_r, e_s, e_r, c_s, c_r, d_s, d_r, f_s, f_r,
    g_s, g_r, t_s, t_r,
):
    T, DI = feats.shape
    H = states.shape[1]
    nh, nz, nx = 2 * nr, ns // 2, nr // 2
    hb, cw = H // nh, DI // nr
    s, r = lax.axis_index("seq"), lax.axis_index("rep")
    z, y, x, c = s // 2, s % 2, r // 2, r % 2
    k = 2 * r + y
    me = s * nr + r
    unsent = []

    def place(a, b):
        return {"seq": a, "rep": b}

    def at(plane, j):
        return place(2 * plane + j % 2, j // 2)

    def send(src, dst, ssem, rsem, where):
        pltpu.make_async_remote_copy(
            src_ref=src, dst_ref=dst, send_sem=ssem, recv_sem=rsem,
            device_id=where, device_id_type=pl.DeviceIdType.MESH,
        ).start()

    def local(src, dst, rsem):
        pltpu.make_async_copy(src, dst, rsem).start()

    def landed(dst, sem):
        pltpu.make_async_copy(dst, dst, sem).wait()

    def send_if(allowed, src, dst, ssem, rsem, where):
        @pl.when(allowed)
        def _():
            send(src, dst, ssem, rsem, where)

        unsent.append((allowed, src, ssem))

    def send_or_local(src, dst, ssem, rsem, where, here):
        send_if(jnp.logical_not(here), src, dst, ssem, rsem, where)

        @pl.when(here)
        def _():
            local(src, dst, rsem)

    def rows(ref, block, count):
        return ref.at[pl.ds(pl.multiple_of(block * count, count), count), :]

    for j in range(nh):
        pay_src[j, :, :hb] = states[:, j * hb : (j + 1) * hb].astype(BF16)
        pay_src[j, :, hb:] = upstream[:, j * hb : (j + 1) * hb]
        tail_src[j, 0:8, :] = states[T - 8 : T, j * hb : (j + 1) * hb]
        tail_src[j, 8:16, :] = jnp.broadcast_to(ids[0:1, T - 1 : T].astype(F32), (8, hb))
    ids_src[...] = jnp.broadcast_to(ids[...].astype(F32), ids_src.shape)

    barrier = pltpu.get_barrier_semaphore()

    def greet(d, _):
        @pl.when(d != me)
        def _():
            pl.semaphore_signal(
                barrier, inc=1, device_id=place(d // nr, d % nr), device_id_type=pl.DeviceIdType.MESH
            )

        return 0

    lax.fori_loop(0, ns * nr, greet, 0)
    pl.semaphore_wait(barrier, ns * nr - 1)

    partner = place(s, r + 1 - 2 * c)
    local(feats, rows(x_all, k, T), x_s0)

    def share(step, src, dx, dy):
        x0, y0 = (x + dx) % nx, (y + dy) % 2
        slot = 2 * (2 * x0 + c) + y0
        dst = rows(x_all, slot, T)
        src = dst if src is None else src
        if dy == 0 or dx == 0:
            for other in range(1, nx):
                if dx == 0:
                    allowed = True if dy == 0 else c == 0
                    send_if(
                        allowed, src, dst, x_sx.at[step * nx + other], x_r.at[slot],
                        place(s, 2 * ((x + other) % nx) + c),
                    )
            if dy == 0:
                allowed = True if dx == 0 else c == 1
                send_if(allowed, src, dst, x_sy.at[step], x_r.at[slot], place(2 * z + 1 - y, r))
        send_if(True, src, dst, x_sd.at[step], x_r.at[slot], partner)

    share(0, feats, 0, 0)

    for i in range(GATES):
        b = GATES * s + i
        g, j = b // nh, b % nh
        dst = w_all.at[
            pl.ds(pl.multiple_of(g * hb, hb), hb), pl.ds(pl.multiple_of(r * cw, cw), cw)
        ]
        for step in range(nz):
            plane = (z + step) % nz
            here = jnp.logical_and(step == 0, j == k)
            send_or_local(
                weight.at[i * hb : (i + 1) * hb, :], dst, w_s.at[i * nz + step],
                w_r.at[g * nr + r], at(plane, j), here,
            )
    for j in range(nh):
        send_or_local(ids_src, ids_all.at[k], i_s.at[j], i_r.at[k], at(z, j), k == j)
        send_or_local(pay_src.at[j], pay.at[k], p_s.at[j], p_r.at[k], at(z, j), k == j)
        send_if(
            jnp.logical_and(y == 1, z < nz - 1), tail_src.at[j], tail_in.at[r], e_s.at[j], e_r.at[r],
            at(z + 1, j),
        )

    hops = [(dx, dy) for dx in range(nx) for dy in range(2)]
    hops.sort(key=lambda hop: (hop[0] > 0) + hop[1])
    for step, (dx, dy) in enumerate(hops):
        if step > 0:
            slot = 2 * (2 * ((x + dx) % nx) + c) + (y + dy) % 2
            landed(rows(x_all, slot, T), x_r.at[slot])
            share(step, None, dx, dy)

    stride = T + 8
    for m in range(nh):
        base = m * stride + 8
        landed(ids_all.at[m], i_r.at[m])
        landed(pay.at[m], p_r.at[m])
        prev[base : base + T, :] = pay[m, :, :hb].astype(F32)
        up[m * T : (m + 1) * T, :] = pay[m, :, hb:].astype(F32)
        ids_col[base : base + T, :] = jnp.broadcast_to(ids_all[m, 0:1, :], (hb, T)).T
        if m % 2:
            before = base - stride + T
            prev[base - 8 : base, :] = prev[before - 8 : before, :]
            ids_col[base - 8 : base, :] = ids_col[before - 8 : before, :]
        else:

            @pl.when(z > 0)
            def _():
                landed(tail_in.at[m // 2], e_r.at[m // 2])
                prev[base - 8 : base, :] = tail_in[m // 2, 0:8, :]
                ids_col[base - 8 : base, :] = tail_in[m // 2, 8:16, :]

            @pl.when(z == 0)
            def _():
                prev[base - 8 : base, :] = jnp.zeros((8, hb), F32)
                ids_col[base - 8 : base, :] = jnp.full((8, hb), -1.0, F32)

    for g in range(GATES):
        for col in range(nr):
            landed(
                w_all.at[g * hb : (g + 1) * hb, col * cw : (col + 1) * cw], w_r.at[g * nr + col]
            )
    landed(rows(x_all, k, T), x_s0)
    for x0 in range(nx):
        for y0 in range(2):
            slot = 2 * (2 * x0 + 1 - c) + y0
            landed(rows(x_all, slot, T), x_r.at[slot])

    group = pl.ds(pl.multiple_of(k * hb, hb), hb)
    rz, rr, rc = (recur[i : i + 1, group] for i in range(GATES))
    bz, br, bc = (bias[i : i + 1, group] for i in range(GATES))
    for m in range(nh):
        span = slice(m * T, (m + 1) * T)
        base = m * stride + 8
        pre = lax.dot_general(
            x_all[span, :], w_all[...], (((1,), (1,)), ((), ())), preferred_element_type=F32
        )
        same = jnp.where(
            ids_col[base : base + T, :] == ids_col[base - 1 : base - 1 + T, :], 1.0, 0.0
        )
        prior = prev[base - 1 : base - 1 + T, :] * same
        gz = jax.nn.sigmoid(pre[:, :hb] + rz * prior + bz)
        gr = jax.nn.sigmoid(pre[:, hb : 2 * hb] + rr * prior + br)
        rp = gr * prior
        gc = jnp.tanh(pre[:, 2 * hb :] + rc * rp + bc)
        az = (gc - prior) * gz * (1.0 - gz)
        ac = gz * (1.0 - gc * gc)
        slope = rp * (1.0 - gr)
        acr = ac * rc
        co_z[span, :] = az
        co_c[span, :] = ac
        co_r[span, :] = acr * slope
        rprior[span, :] = rp
        prior_all[span, :] = prior
        jac[span, :] = same * (1.0 - gz + az * rz + acr * (gr + slope * rr))

    def back(i, state):
        a, b = state
        t = T - 1 - i
        f = jac[pl.ds(t, nh, stride=T), :]
        b = b + up[pl.ds(t, nh, stride=T), :]
        scan_a[t] = a
        scan_b[t] = b
        return f * a, f * b

    a, b = lax.fori_loop(0, T, back, (jnp.ones((nh, hb), F32), jnp.zeros((nh, hb), F32)), unroll=8)
    seg_out[...] = jnp.zeros(seg_out.shape, F32)
    for o in range(nr):
        first, second = slice(2 * o, 2 * o + 1), slice(2 * o + 1, 2 * o + 2)
        seg_out[0, o : o + 1, :] = a[first, :] * a[second, :]
        seg_out[1, o : o + 1, :] = b[first, :] + a[first, :] * b[second, :]
    for plane in range(nz - 1):
        send_if(plane < z, seg_out, seg_in.at[z], c_s.at[plane], c_r.at[z], at(plane, k))
    carry[...] = jnp.zeros(carry.shape, F32)
    for plane in reversed(range(1, nz)):

        @pl.when(plane > z)
        def _():
            landed(seg_in.at[plane], c_r.at[plane])
            carry[0:nr, :] = seg_in[plane, 1, 0:nr, :] + seg_in[plane, 0, 0:nr, :] * carry[0:nr, :]

    into = carry[0:nr, :]
    carry_rows = []
    for o in range(nr):
        later = into[o : o + 1, :]
        second = slice(2 * o + 1, 2 * o + 2)
        carry_rows += [b[second, :] + a[second, :] * later, later]
    carried = jnp.concatenate(carry_rows, 0)

    def finish(t, _):
        lam[pl.ds(t, nh, stride=T), :] = scan_b[t] + scan_a[t] * carried
        return 0

    lax.fori_loop(0, T, finish, 0, unroll=8)

    sums = [jnp.zeros((1, hb), F32) for _ in range(6)]
    for m in range(nh):
        span = slice(m * T, (m + 1) * T)
        prior = prior_all[span, :]
        adj = lam[span, :]
        grad_z = adj * co_z[span, :]
        grad_r = adj * co_r[span, :]
        grad_c = adj * co_c[span, :]
        grads[span, :hb] = grad_z.astype(BF16)
        grads[span, hb : 2 * hb] = grad_r.astype(BF16)
        grads[span, 2 * hb :] = grad_c.astype(BF16)
        terms = (grad_z, grad_r, grad_c, grad_z * prior, grad_r * prior, grad_c * rprior[span, :])
        sums = [total + jnp.sum(term, 0, keepdims=True) for total, term in zip(sums, terms)]
    for i in range(6):
        st_out[i : i + 1, :] = sums[i]
    st_out[6:8, :] = jnp.zeros((2, hb), F32)

    for g in range(GATES):
        wg_out[g] = lax.dot_general(
            grads[:, g * hb : (g + 1) * hb], x_all[...], (((0,), (0,)), ((), ())),
            preferred_element_type=F32,
        ).astype(BF16)
        b = g * nh + k
        owner, i = b // GATES, b % GATES
        for col in range(nr):
            here = jnp.logical_and(owner == s, r == col)
            send_or_local(
                wg_out.at[g, :, col * cw : (col + 1) * cw], wg_in.at[z * GATES + i],
                g_s.at[g * nr + col], g_r.at[z * GATES + i], place(owner, col), here,
            )

    chips = [(x0, y0) for x0 in range(nx) for y0 in range(2)]
    for n, (x0, y0) in enumerate(chips):
        part_out[n] = jnp.dot(
            rows(grads, 2 * (2 * x0 + 1 - c) + y0, T)[...], w_all[...], preferred_element_type=F32
        ).astype(BF16)
        send_if(True, part_out.at[n], part_in.at[n], d_s.at[n], d_r.at[n], partner)
    for n, (x0, y0) in enumerate(chips):
        part_keep[n] = jnp.dot(
            rows(grads, 2 * (2 * x0 + c) + y0, T)[...], w_all[...], preferred_element_type=F32
        )
    chip = 2 * x + y
    for n, (x0, y0) in enumerate(chips):
        landed(part_in.at[n], d_r.at[n])
        fin_out[n] = (part_keep[n] + part_in[n].astype(F32)).astype(BF16)
        send_or_local(
            fin_out.at[n], fin_in.at[chip], f_s.at[n], f_r.at[chip],
            place(2 * z + y0, 2 * x0 + c), chip == n,
        )

    slot = k * nz + z
    st_in[slot] = st_out[...]

    def tell(d, _):
        @pl.when(d != me)
        def _():
            send(st_out, st_in.at[slot], t_s.at[d], t_r.at[slot], place(d // nr, d % nr))

        return 0

    lax.fori_loop(0, ns * nr, tell, 0)

    scale = 1.0 / math.sqrt(ns * nr * T)

    def heard(d, _):
        @pl.when(d != slot)
        def _():
            landed(st_in.at[d], t_r.at[d])

        return 0

    lax.fori_loop(0, ns * nr, heard, 0)
    for j in range(nh):
        total = st_in[j * nz]
        for other in range(1, nz):
            total = total + st_in[j * nz + other]
        out_p[:, j * hb : (j + 1) * hb] = total[:6] * scale

    total = None
    for n in range(len(chips)):
        landed(fin_in.at[n], f_r.at[n])
        term = fin_in[n].astype(F32)
        total = term if total is None else total + term
    out_in[...] = total.astype(BF16)

    for i in range(GATES):
        total = None
        for other in range(nz):
            landed(wg_in.at[other * GATES + i], g_r.at[other * GATES + i])
            term = wg_in[other * GATES + i].astype(F32)
            total = term if total is None else total + term
        out_w[i * hb : (i + 1) * hb, :] = total * scale

    def told(d, _):
        @pl.when(d != me)
        def _():
            landed(st_out, t_s.at[d])

        return 0

    lax.fori_loop(0, ns * nr, told, 0)
    for sent, src, sem in unsent:
        if sent is True:
            landed(src, sem)
        else:

            @pl.when(sent)
            def _():
                landed(src, sem)


def by_hidden(ns, nr, inputs, weight_t, states, doc_ids, recur, bias, out_grad):
    T, DI = inputs.shape[1:]
    H = states.shape[2]
    nh, nz, nx = 2 * nr, ns // 2, nr // 2
    hb, cw = H // nh, DI // nr
    L = nh * T
    vm = pltpu.VMEM
    scratch = [
        vm((nh, T, 2 * hb), BF16),
        vm((nh, T, 2 * hb), BF16),
        vm((8, T), F32),
        vm((nh, 8, T), F32),
        vm((nh, 16, hb), F32),
        vm((nr, 16, hb), F32),
        vm((L, DI), BF16),
        vm((GATES * hb, DI), BF16),
        vm((L + 8 * nh, hb), F32),
        vm((L + 8 * nh, hb), F32),
        vm((L, hb), F32),
        vm((L, hb), F32),
        vm((L, hb), F32),
        vm((L, hb), F32),
        vm((L, hb), F32),
        vm((L, hb), F32),
        vm((L, hb), F32),
        vm((T, nh, hb), F32),
        vm((T, nh, hb), F32),
        vm((nh, hb), F32),
        vm((2, 8, hb), F32),
        vm((nz, 2, 8, hb), F32),
        vm((L, hb), F32),
        vm((L, GATES * hb), BF16),
        vm((nr, T, DI), BF16),
        vm((nr, T, DI), BF16),
        vm((nr, T, DI), F32),
        vm((nr, T, DI), BF16),
        vm((nr, T, DI), BF16),
        vm((GATES, hb, DI), BF16),
        vm((nz * GATES, hb, cw), BF16),
        vm((8, hb), F32),
        vm((ns * nr, 8, hb), F32),
    ]
    dma = pltpu.SemaphoreType.DMA
    counts = [
        None, nr * nx, nr, nr, nh, GATES * nz, GATES * nr, nh, nh, nh, nh, nh, nr, nz, nz, nr, nr, nr, nr,
        GATES * nr, GATES * nz, ns * nr, ns * nr,
    ]
    sems = [dma if n is None else dma((n,)) for n in counts]
    whole = pl.BlockSpec(memory_space=pltpu.VMEM)
    out_in, out_w, out_p = pl.pallas_call(
        functools.partial(kernel, ns, nr),
        out_shape=(
            jax.ShapeDtypeStruct((T, DI), BF16),
            jax.ShapeDtypeStruct(weight_t.shape, F32),
            jax.ShapeDtypeStruct((6, H), F32),
        ),
        in_specs=[whole] * 7,
        out_specs=(whole,) * 3,
        scratch_shapes=scratch + sems,
        compiler_params=pltpu.CompilerParams(
            collective_id=0, has_side_effects=True, vmem_limit_bytes=56 * 1024 * 1024
        ),
    )(inputs[0], weight_t, states[0], doc_ids, recur, bias, out_grad[0])
    return out_in[None], out_w, out_p


def fits(ns, nr, inputs, weight_t, states):
    parts, L, DI = inputs.shape
    H = states.shape[2]
    return (
        parts == nr
        and ns == 2 * nr
        and ns % 8 == 0
        and ns == 8
        and H % (ns * 128) == 0
        and DI % (nr * 128) == 0
        and L % (ns * 128) == 0
        and L * DI <= 1 << 21
    )


def solution(mesh):
    ns, nr = mesh.shape["seq"], mesh.shape["rep"]
    placed = (
        P("rep", "seq", None),
        P("seq", "rep"),
        P("rep", "seq", None),
        P("rep", "seq"),
        P(),
        P(),
        P("rep", "seq", None),
    )

    def run(inputs, weight_t, states, doc_ids, recur, bias, out_grad):
        kernelized = fits(ns, nr, inputs, weight_t, states)
        body = functools.partial(by_hidden, ns, nr) if kernelized else by_tokens
        return jax.shard_map(
            body,
            mesh=mesh,
            in_specs=placed,
            out_specs=(P("rep", "seq", None), P("seq", "rep"), P()),
            check_vma=False,
        )(inputs, weight_t, states, doc_ids, recur, bias, out_grad)

    return run
```

```python
import functools
import math

import jax
import jax.numpy as jnp
from jax import lax
from jax.experimental import pallas as pl
from jax.experimental.pallas import tpu as pltpu
from jax.sharding import PartitionSpec as P

F32 = jnp.float32
BF16 = jnp.bfloat16
GATES = 3


def shifted(block, axis, distance):
    devices = range(lax.axis_size(axis))
    route = [(i - distance, i) for i in devices if i - distance in devices]
    return lax.ppermute(block, axis, route)


def compose(earlier, later):
    return (later[0] * earlier[0], later[1] + later[0] * earlier[1])


def by_tokens(inputs, weight_t, states, doc_ids, recur, bias, out_grad):
    feats = inputs[0]
    hidden_now = states[0]
    ids_float = doc_ids[0].astype(F32)
    count = feats.shape[0]
    width = hidden_now.shape[1]
    columns = lax.all_gather(weight_t, "rep", axis=1, tiled=True)
    contract_last = (((1,), (1,)), ((), ()))
    full_weight = lax.all_gather(columns, "seq", axis=0, tiled=True)
    preact = lax.dot_general(feats, full_weight, contract_last, preferred_element_type=F32)
    tail_state, tail_id = shifted((hidden_now[-1:], ids_float[-1:]), "seq", 1)
    first_same = jnp.where(
        (ids_float[0] == tail_id[0]) & (lax.axis_index("seq") > 0), 1.0, 0.0
    ).astype(F32)
    same = jnp.concatenate([first_same[None], (ids_float[1:] == ids_float[:-1]).astype(F32)])
    prior = jnp.concatenate([tail_state, hidden_now[:-1]], 0) * same[:, None]
    gate_z = jax.nn.sigmoid(preact[:, :width] + recur[0] * prior + bias[0])
    gate_r = jax.nn.sigmoid(preact[:, width : 2 * width] + recur[1] * prior + bias[1])
    gate_c = jnp.tanh(preact[:, 2 * width :] + recur[2] * gate_r * prior + bias[2])
    jacobian = same[:, None] * (
        1.0
        - gate_z
        + (gate_c - prior) * gate_z * (1.0 - gate_z) * recur[0]
        + gate_z
        * (1.0 - gate_c * gate_c)
        * recur[2]
        * (gate_r + prior * gate_r * (1.0 - gate_r) * recur[1])
    )
    upstream = out_grad[0].astype(F32)
    jac_rows, up_rows = (
        lax.all_to_all(jacobian.T, "seq", split_axis=0, concat_axis=1, tiled=True),
        lax.all_to_all(upstream.T, "seq", split_axis=0, concat_axis=1, tiled=True),
    )
    factor = jnp.concatenate([jac_rows[:, 1:], jnp.zeros((jac_rows.shape[0], 1), F32)], 1)
    _, adjoint_rows = lax.associative_scan(compose, (factor, up_rows), reverse=True, axis=1)
    adjoint = lax.all_to_all(adjoint_rows, "seq", split_axis=1, concat_axis=0, tiled=True).T
    grad_z = adjoint * (gate_c - prior) * gate_z * (1.0 - gate_z)
    grad_c = adjoint * gate_z * (1.0 - gate_c * gate_c)
    grad_r = grad_c * recur[2] * prior * gate_r * (1.0 - gate_r)
    grad_pre = jnp.concatenate([grad_z, grad_r, grad_c], 1).astype(BF16)
    input_grad = jnp.dot(grad_pre, full_weight, preferred_element_type=F32)
    tokens_all = count * inputs.shape[0] * lax.axis_size("seq") * lax.axis_size("rep")
    normal_factor = 1.0 / math.sqrt(tokens_all)
    row_share = lax.psum_scatter(
        lax.dot_general(grad_pre, feats, (((0,), (0,)), ((), ())), preferred_element_type=F32),
        "seq",
        scatter_dimension=0,
        tiled=True,
    )
    weight_grad = (
        lax.psum_scatter(row_share.astype(BF16), "rep", scatter_dimension=1, tiled=True).astype(F32)
        * normal_factor
    )
    stats = jnp.stack(
        [
            grad_z.sum(0),
            grad_r.sum(0),
            grad_c.sum(0),
            (grad_z * prior).sum(0),
            (grad_r * prior).sum(0),
            (grad_c * gate_r * prior).sum(0),
        ]
    )
    param_grad = lax.psum(stats, ("seq", "rep")) * normal_factor
    return (input_grad.astype(BF16)[None], weight_grad, param_grad)


def kernel(
    ns, nr, feats, weight, states, ids, recur, bias, upstream,
    out_in, out_w, out_p,
    pay_src, pay, ids_src, ids_all, tail_src, tail_in, x_all, w_all, prev, ids_col, up, jac,
    co_z, co_r, co_c, rprior, prior_all,
    scan_a, scan_b, carry, seg_out, seg_in, lam, grads, part_out, part_in, part_keep, fin_out, fin_in,
    wg_out, wg_in, st_out, st_in,
    x_s0, x_sx, x_sy, x_sd, x_r, w_s, w_r, p_s, p_r, i_s, i_r, e_s, e_r, c_s, c_r, d_s, d_r, f_s, f_r,
    g_s, g_r, t_s, t_r,
):
    T, DI = feats.shape
    H = states.shape[1]
    nh, nz, nx = 2 * nr, ns // 2, nr // 2
    hb, cw = H // nh, DI // nr
    s, r = lax.axis_index("seq"), lax.axis_index("rep")
    z, y, x, c = s // 2, s % 2, r // 2, r % 2
    k = 2 * r + y
    me = s * nr + r
    unsent = []

    def place(a, b):
        return {"seq": a, "rep": b}

    def at(plane, j):
        return place(2 * plane + j % 2, j // 2)

    def send(src, dst, ssem, rsem, where):
        pltpu.make_async_remote_copy(
            src_ref=src, dst_ref=dst, send_sem=ssem, recv_sem=rsem,
            device_id=where, device_id_type=pl.DeviceIdType.MESH,
        ).start()

    def local(src, dst, rsem):
        pltpu.make_async_copy(src, dst, rsem).start()

    def landed(dst, sem):
        pltpu.make_async_copy(dst, dst, sem).wait()

    def send_if(allowed, src, dst, ssem, rsem, where):
        @pl.when(allowed)
        def _():
            send(src, dst, ssem, rsem, where)

        unsent.append((allowed, src, ssem))

    def send_or_local(src, dst, ssem, rsem, where, here):
        send_if(jnp.logical_not(here), src, dst, ssem, rsem, where)

        @pl.when(here)
        def _():
            local(src, dst, rsem)

    def rows(ref, block, count):
        return ref.at[pl.ds(pl.multiple_of(block * count, count), count), :]

    barrier = pltpu.get_barrier_semaphore()

    def greet(d, _):
        @pl.when(d != me)
        def _():
            pl.semaphore_signal(
                barrier, inc=1, device_id=place(d // nr, d % nr), device_id_type=pl.DeviceIdType.MESH
            )

        return 0

    lax.fori_loop(0, ns * nr, greet, 0)
    for j in range(nh):
        pay_src[j, :, :hb] = states[:, j * hb : (j + 1) * hb].astype(BF16)
        pay_src[j, :, hb:] = upstream[:, j * hb : (j + 1) * hb]
        tail_src[j, 0:8, :] = states[T - 8 : T, j * hb : (j + 1) * hb]
        tail_src[j, 8:16, :] = jnp.broadcast_to(ids[0:1, T - 1 : T].astype(F32), (8, hb))
    ids_src[...] = jnp.broadcast_to(ids[...].astype(F32), ids_src.shape)

    pl.semaphore_wait(barrier, ns * nr - 1)

    steps = sorted(range(nz), key=lambda step: -min(step, nz - step))
    for step in steps:
        plane = (z + step) % nz
        for i in range(GATES):
            b = GATES * s + i
            g, j = b // nh, b % nh
            dst = w_all.at[
                pl.ds(pl.multiple_of(g * hb, hb), hb), pl.ds(pl.multiple_of(r * cw, cw), cw)
            ]
            here = jnp.logical_and(step == 0, j == k)
            send_or_local(
                weight.at[i * hb : (i + 1) * hb, :], dst, w_s.at[i * nz + step],
                w_r.at[g * nr + r], at(plane, j), here,
            )
    partner = place(s, r + 1 - 2 * c)
    local(feats, rows(x_all, k, T), x_s0)

    def share(step, src, dx, dy):
        x0, y0 = (x + dx) % nx, (y + dy) % 2
        slot = 2 * (2 * x0 + c) + y0
        dst = rows(x_all, slot, T)
        src = dst if src is None else src
        if dy == 0 or dx == 0:
            for other in range(1, nx):
                if dx == 0:
                    allowed = True if dy == 0 else c == 0
                    send_if(
                        allowed, src, dst, x_sx.at[step * nx + other], x_r.at[slot],
                        place(s, 2 * ((x + other) % nx) + c),
                    )
            if dy == 0:
                allowed = True if dx == 0 else c == 1
                send_if(allowed, src, dst, x_sy.at[step], x_r.at[slot], place(2 * z + 1 - y, r))
        send_if(True, src, dst, x_sd.at[step], x_r.at[slot], partner)

    share(0, feats, 0, 0)

    for j in range(nh):
        send_or_local(ids_src, ids_all.at[k], i_s.at[j], i_r.at[k], at(z, j), k == j)
        send_or_local(pay_src.at[j], pay.at[k], p_s.at[j], p_r.at[k], at(z, j), k == j)
        send_if(
            jnp.logical_and(y == 1, z < nz - 1), tail_src.at[j], tail_in.at[r], e_s.at[j], e_r.at[r],
            at(z + 1, j),
        )

    hops = [(dx, dy) for dx in range(nx) for dy in range(2)]
    hops.sort(key=lambda hop: (hop[0] > 0) + hop[1])
    for step, (dx, dy) in enumerate(hops):
        if step > 0:
            slot = 2 * (2 * ((x + dx) % nx) + c) + (y + dy) % 2
            landed(rows(x_all, slot, T), x_r.at[slot])
            share(step, None, dx, dy)

    stride = T + 8
    for m in range(nh):
        base = m * stride + 8
        landed(ids_all.at[m], i_r.at[m])
        landed(pay.at[m], p_r.at[m])
        prev[base : base + T, :] = pay[m, :, :hb].astype(F32)
        up[m * T : (m + 1) * T, :] = pay[m, :, hb:].astype(F32)
        ids_col[base : base + T, :] = jnp.broadcast_to(ids_all[m, 0:1, :], (hb, T)).T
        if m % 2:
            before = base - stride + T
            prev[base - 8 : base, :] = prev[before - 8 : before, :]
            ids_col[base - 8 : base, :] = ids_col[before - 8 : before, :]
        else:

            @pl.when(z > 0)
            def _():
                landed(tail_in.at[m // 2], e_r.at[m // 2])
                prev[base - 8 : base, :] = tail_in[m // 2, 0:8, :]
                ids_col[base - 8 : base, :] = tail_in[m // 2, 8:16, :]

            @pl.when(z == 0)
            def _():
                prev[base - 8 : base, :] = jnp.zeros((8, hb), F32)
                ids_col[base - 8 : base, :] = jnp.full((8, hb), -1.0, F32)

    for g in range(GATES):
        for col in range(nr):
            landed(
                w_all.at[g * hb : (g + 1) * hb, col * cw : (col + 1) * cw], w_r.at[g * nr + col]
            )
    landed(rows(x_all, k, T), x_s0)
    for x0 in range(nx):
        for y0 in range(2):
            slot = 2 * (2 * x0 + 1 - c) + y0
            landed(rows(x_all, slot, T), x_r.at[slot])

    group = pl.ds(pl.multiple_of(k * hb, hb), hb)
    rz, rr, rc = (recur[i : i + 1, group] for i in range(GATES))
    bz, br, bc = (bias[i : i + 1, group] for i in range(GATES))
    for m in range(nh):
        span = slice(m * T, (m + 1) * T)
        base = m * stride + 8
        pre = lax.dot_general(
            x_all[span, :], w_all[...], (((1,), (1,)), ((), ())), preferred_element_type=F32
        )
        same = jnp.where(
            ids_col[base : base + T, :] == ids_col[base - 1 : base - 1 + T, :], 1.0, 0.0
        )
        prior = prev[base - 1 : base - 1 + T, :] * same
        gz = jax.nn.sigmoid(pre[:, :hb] + rz * prior + bz)
        gr = jax.nn.sigmoid(pre[:, hb : 2 * hb] + rr * prior + br)
        rp = gr * prior
        gc = jnp.tanh(pre[:, 2 * hb :] + rc * rp + bc)
        az = (gc - prior) * gz * (1.0 - gz)
        ac = gz * (1.0 - gc * gc)
        slope = rp * (1.0 - gr)
        acr = ac * rc
        co_z[span, :] = az
        co_c[span, :] = ac
        co_r[span, :] = acr * slope
        rprior[span, :] = rp
        prior_all[span, :] = prior
        jac[span, :] = same * (1.0 - gz + az * rz + acr * (gr + slope * rr))

    def back(i, state):
        a, b = state
        t = T - 1 - i
        f = jac[pl.ds(t, nh, stride=T), :]
        b = b + up[pl.ds(t, nh, stride=T), :]
        scan_a[t] = a
        scan_b[t] = b
        return f * a, f * b

    a, b = lax.fori_loop(0, T, back, (jnp.ones((nh, hb), F32), jnp.zeros((nh, hb), F32)), unroll=8)
    seg_out[...] = jnp.zeros(seg_out.shape, F32)
    for o in range(nr):
        first, second = slice(2 * o, 2 * o + 1), slice(2 * o + 1, 2 * o + 2)
        seg_out[0, o : o + 1, :] = a[first, :] * a[second, :]
        seg_out[1, o : o + 1, :] = b[first, :] + a[first, :] * b[second, :]
    for plane in range(nz - 1):
        send_if(plane < z, seg_out, seg_in.at[z], c_s.at[plane], c_r.at[z], at(plane, k))
    carry[...] = jnp.zeros(carry.shape, F32)
    for plane in reversed(range(1, nz)):

        @pl.when(plane > z)
        def _():
            landed(seg_in.at[plane], c_r.at[plane])
            carry[0:nr, :] = seg_in[plane, 1, 0:nr, :] + seg_in[plane, 0, 0:nr, :] * carry[0:nr, :]

    into = carry[0:nr, :]
    carry_rows = []
    for o in range(nr):
        later = into[o : o + 1, :]
        second = slice(2 * o + 1, 2 * o + 2)
        carry_rows += [b[second, :] + a[second, :] * later, later]
    carried = jnp.concatenate(carry_rows, 0)

    def finish(t, _):
        lam[pl.ds(t, nh, stride=T), :] = scan_b[t] + scan_a[t] * carried
        return 0

    lax.fori_loop(0, T, finish, 0, unroll=8)

    sums = [jnp.zeros((1, hb), F32) for _ in range(6)]
    for m in range(nh):
        span = slice(m * T, (m + 1) * T)
        prior = prior_all[span, :]
        adj = lam[span, :]
        grad_z = adj * co_z[span, :]
        grad_r = adj * co_r[span, :]
        grad_c = adj * co_c[span, :]
        grads[span, :hb] = grad_z.astype(BF16)
        grads[span, hb : 2 * hb] = grad_r.astype(BF16)
        grads[span, 2 * hb :] = grad_c.astype(BF16)
        terms = (grad_z, grad_r, grad_c, grad_z * prior, grad_r * prior, grad_c * rprior[span, :])
        sums = [total + jnp.sum(term, 0, keepdims=True) for total, term in zip(sums, terms)]
    for i in range(6):
        st_out[i : i + 1, :] = sums[i]
    st_out[6:8, :] = jnp.zeros((2, hb), F32)

    slot = k * nz + z
    st_in[slot] = st_out[...]

    def tell(d, _):
        @pl.when(d != me)
        def _():
            send(st_out, st_in.at[slot], t_s.at[d], t_r.at[slot], place(d // nr, d % nr))

        return 0

    lax.fori_loop(0, ns * nr, tell, 0)

    for g in range(GATES):
        wg_out[g] = lax.dot_general(
            grads[:, g * hb : (g + 1) * hb], x_all[...], (((0,), (0,)), ((), ())),
            preferred_element_type=F32,
        ).astype(BF16)
        b = g * nh + k
        owner, i = b // GATES, b % GATES
        for col in range(nr):
            here = jnp.logical_and(owner == s, r == col)
            send_or_local(
                wg_out.at[g, :, col * cw : (col + 1) * cw], wg_in.at[z * GATES + i],
                g_s.at[g * nr + col], g_r.at[z * GATES + i], place(owner, col), here,
            )

    chips = [(x0, y0) for x0 in range(nx) for y0 in range(2)]
    for n, (x0, y0) in enumerate(chips):
        part_out[n] = jnp.dot(
            rows(grads, 2 * (2 * x0 + 1 - c) + y0, T)[...], w_all[...], preferred_element_type=F32
        ).astype(BF16)
        send_if(True, part_out.at[n], part_in.at[n], d_s.at[n], d_r.at[n], partner)
    for n, (x0, y0) in enumerate(chips):
        part_keep[n] = jnp.dot(
            rows(grads, 2 * (2 * x0 + c) + y0, T)[...], w_all[...], preferred_element_type=F32
        )
    chip = 2 * x + y
    for n, (x0, y0) in enumerate(chips):
        landed(part_in.at[n], d_r.at[n])
        fin_out[n] = (part_keep[n] + part_in[n].astype(F32)).astype(BF16)
        send_or_local(
            fin_out.at[n], fin_in.at[chip], f_s.at[n], f_r.at[chip],
            place(2 * z + y0, 2 * x0 + c), chip == n,
        )

    scale = 1.0 / math.sqrt(ns * nr * T)

    def heard(d, _):
        @pl.when(d != slot)
        def _():
            landed(st_in.at[d], t_r.at[d])

        return 0

    lax.fori_loop(0, ns * nr, heard, 0)
    for j in range(nh):
        total = st_in[j * nz]
        for other in range(1, nz):
            total = total + st_in[j * nz + other]
        out_p[:, j * hb : (j + 1) * hb] = total[:6] * scale

    total = None
    for n in range(len(chips)):
        landed(fin_in.at[n], f_r.at[n])
        term = fin_in[n].astype(F32)
        total = term if total is None else total + term
    out_in[...] = total.astype(BF16)

    for i in range(GATES):
        total = None
        for other in range(nz):
            landed(wg_in.at[other * GATES + i], g_r.at[other * GATES + i])
            term = wg_in[other * GATES + i].astype(F32)
            total = term if total is None else total + term
        out_w[i * hb : (i + 1) * hb, :] = total * scale

    def told(d, _):
        @pl.when(d != me)
        def _():
            landed(st_out, t_s.at[d])

        return 0

    lax.fori_loop(0, ns * nr, told, 0)
    for sent, src, sem in unsent:
        if sent is True:
            landed(src, sem)
        else:

            @pl.when(sent)
            def _():
                landed(src, sem)


def by_hidden(ns, nr, inputs, weight_t, states, doc_ids, recur, bias, out_grad):
    T, DI = inputs.shape[1:]
    H = states.shape[2]
    nh, nz, nx = 2 * nr, ns // 2, nr // 2
    hb, cw = H // nh, DI // nr
    L = nh * T
    vm = pltpu.VMEM
    scratch = [
        vm((nh, T, 2 * hb), BF16),
        vm((nh, T, 2 * hb), BF16),
        vm((8, T), F32),
        vm((nh, 8, T), F32),
        vm((nh, 16, hb), F32),
        vm((nr, 16, hb), F32),
        vm((L, DI), BF16),
        vm((GATES * hb, DI), BF16),
        vm((L + 8 * nh, hb), F32),
        vm((L + 8 * nh, hb), F32),
        vm((L, hb), F32),
        vm((L, hb), F32),
        vm((L, hb), F32),
        vm((L, hb), F32),
        vm((L, hb), F32),
        vm((L, hb), F32),
        vm((L, hb), F32),
        vm((T, nh, hb), F32),
        vm((T, nh, hb), F32),
        vm((nh, hb), F32),
        vm((2, 8, hb), F32),
        vm((nz, 2, 8, hb), F32),
        vm((L, hb), F32),
        vm((L, GATES * hb), BF16),
        vm((nr, T, DI), BF16),
        vm((nr, T, DI), BF16),
        vm((nr, T, DI), F32),
        vm((nr, T, DI), BF16),
        vm((nr, T, DI), BF16),
        vm((GATES, hb, DI), BF16),
        vm((nz * GATES, hb, cw), BF16),
        vm((8, hb), F32),
        vm((ns * nr, 8, hb), F32),
    ]
    dma = pltpu.SemaphoreType.DMA
    counts = [
        None, nr * nx, nr, nr, nh, GATES * nz, GATES * nr, nh, nh, nh, nh, nh, nr, nz, nz, nr, nr, nr, nr,
        GATES * nr, GATES * nz, ns * nr, ns * nr,
    ]
    sems = [dma if n is None else dma((n,)) for n in counts]
    whole = pl.BlockSpec(memory_space=pltpu.VMEM)
    out_in, out_w, out_p = pl.pallas_call(
        functools.partial(kernel, ns, nr),
        out_shape=(
            jax.ShapeDtypeStruct((T, DI), BF16),
            jax.ShapeDtypeStruct(weight_t.shape, F32),
            jax.ShapeDtypeStruct((6, H), F32),
        ),
        in_specs=[whole] * 7,
        out_specs=(whole,) * 3,
        scratch_shapes=scratch + sems,
        compiler_params=pltpu.CompilerParams(
            collective_id=0, has_side_effects=True, vmem_limit_bytes=56 * 1024 * 1024
        ),
    )(inputs[0], weight_t, states[0], doc_ids, recur, bias, out_grad[0])
    return out_in[None], out_w, out_p


def fits(ns, nr, inputs, weight_t, states):
    parts, L, DI = inputs.shape
    H = states.shape[2]
    return (
        parts == nr
        and ns == 2 * nr
        and ns % 8 == 0
        and ns == 8
        and H % (ns * 128) == 0
        and DI % (nr * 128) == 0
        and L % (ns * 128) == 0
        and L * DI <= 1 << 21
    )


def solution(mesh):
    ns, nr = mesh.shape["seq"], mesh.shape["rep"]
    placed = (
        P("rep", "seq", None),
        P("seq", "rep"),
        P("rep", "seq", None),
        P("rep", "seq"),
        P(),
        P(),
        P("rep", "seq", None),
    )

    def run(inputs, weight_t, states, doc_ids, recur, bias, out_grad):
        kernelized = fits(ns, nr, inputs, weight_t, states)
        body = functools.partial(by_hidden, ns, nr) if kernelized else by_tokens
        return jax.shard_map(
            body,
            mesh=mesh,
            in_specs=placed,
            out_specs=(P("rep", "seq", None), P("seq", "rep"), P()),
            check_vma=False,
        )(inputs, weight_t, states, doc_ids, recur, bias, out_grad)

    return run
```

```python
import functools
import math

import jax
import jax.numpy as jnp
from jax import lax
from jax.experimental import pallas as pl
from jax.experimental.pallas import tpu as pltpu
from jax.sharding import PartitionSpec as P

F32 = jnp.float32
BF16 = jnp.bfloat16
GATES = 3


def shifted(block, axis, distance):
    devices = range(lax.axis_size(axis))
    route = [(i - distance, i) for i in devices if i - distance in devices]
    return lax.ppermute(block, axis, route)


def compose(earlier, later):
    return (later[0] * earlier[0], later[1] + later[0] * earlier[1])


def by_tokens(inputs, weight_t, states, doc_ids, recur, bias, out_grad):
    feats = inputs[0]
    hidden_now = states[0]
    ids_float = doc_ids[0].astype(F32)
    count = feats.shape[0]
    width = hidden_now.shape[1]
    columns = lax.all_gather(weight_t, "rep", axis=1, tiled=True)
    contract_last = (((1,), (1,)), ((), ()))
    full_weight = lax.all_gather(columns, "seq", axis=0, tiled=True)
    preact = lax.dot_general(feats, full_weight, contract_last, preferred_element_type=F32)
    tail_state, tail_id = shifted((hidden_now[-1:], ids_float[-1:]), "seq", 1)
    first_same = jnp.where(
        (ids_float[0] == tail_id[0]) & (lax.axis_index("seq") > 0), 1.0, 0.0
    ).astype(F32)
    same = jnp.concatenate([first_same[None], (ids_float[1:] == ids_float[:-1]).astype(F32)])
    prior = jnp.concatenate([tail_state, hidden_now[:-1]], 0) * same[:, None]
    gate_z = jax.nn.sigmoid(preact[:, :width] + recur[0] * prior + bias[0])
    gate_r = jax.nn.sigmoid(preact[:, width : 2 * width] + recur[1] * prior + bias[1])
    gate_c = jnp.tanh(preact[:, 2 * width :] + recur[2] * gate_r * prior + bias[2])
    jacobian = same[:, None] * (
        1.0
        - gate_z
        + (gate_c - prior) * gate_z * (1.0 - gate_z) * recur[0]
        + gate_z
        * (1.0 - gate_c * gate_c)
        * recur[2]
        * (gate_r + prior * gate_r * (1.0 - gate_r) * recur[1])
    )
    upstream = out_grad[0].astype(F32)
    jac_rows, up_rows = (
        lax.all_to_all(jacobian.T, "seq", split_axis=0, concat_axis=1, tiled=True),
        lax.all_to_all(upstream.T, "seq", split_axis=0, concat_axis=1, tiled=True),
    )
    factor = jnp.concatenate([jac_rows[:, 1:], jnp.zeros((jac_rows.shape[0], 1), F32)], 1)
    _, adjoint_rows = lax.associative_scan(compose, (factor, up_rows), reverse=True, axis=1)
    adjoint = lax.all_to_all(adjoint_rows, "seq", split_axis=1, concat_axis=0, tiled=True).T
    grad_z = adjoint * (gate_c - prior) * gate_z * (1.0 - gate_z)
    grad_c = adjoint * gate_z * (1.0 - gate_c * gate_c)
    grad_r = grad_c * recur[2] * prior * gate_r * (1.0 - gate_r)
    grad_pre = jnp.concatenate([grad_z, grad_r, grad_c], 1).astype(BF16)
    input_grad = jnp.dot(grad_pre, full_weight, preferred_element_type=F32)
    tokens_all = count * inputs.shape[0] * lax.axis_size("seq") * lax.axis_size("rep")
    normal_factor = 1.0 / math.sqrt(tokens_all)
    row_share = lax.psum_scatter(
        lax.dot_general(grad_pre, feats, (((0,), (0,)), ((), ())), preferred_element_type=F32),
        "seq",
        scatter_dimension=0,
        tiled=True,
    )
    weight_grad = (
        lax.psum_scatter(row_share.astype(BF16), "rep", scatter_dimension=1, tiled=True).astype(F32)
        * normal_factor
    )
    stats = jnp.stack(
        [
            grad_z.sum(0),
            grad_r.sum(0),
            grad_c.sum(0),
            (grad_z * prior).sum(0),
            (grad_r * prior).sum(0),
            (grad_c * gate_r * prior).sum(0),
        ]
    )
    param_grad = lax.psum(stats, ("seq", "rep")) * normal_factor
    return (input_grad.astype(BF16)[None], weight_grad, param_grad)


def kernel(
    ns, nr, feats, weight, states, ids, recur, bias, upstream,
    out_in, out_w, out_p,
    pay_src, pay, ids_src, ids_all, tail_src, tail_in, x_all, w_all, prev, ids_col, up, jac,
    co_z, co_r, co_c, rprior, prior_all,
    scan_a, scan_b, carry, seg_out, seg_in, lam, grads, part_out, part_in, part_keep, fin_out, fin_in,
    wg_out, wg_in, st_out, st_in, pre_all,
    x_s0, x_sx, x_sy, x_sd, x_r, w_s, w_r, p_s, p_r, i_s, i_r, e_s, e_r, c_s, c_r, d_s, d_r, f_s, f_r,
    g_s, g_r, t_s, t_r,
):
    T, DI = feats.shape
    H = states.shape[1]
    nh, nz, nx = 2 * nr, ns // 2, nr // 2
    hb, cw = H // nh, DI // nr
    s, r = lax.axis_index("seq"), lax.axis_index("rep")
    z, y, x, c = s // 2, s % 2, r // 2, r % 2
    k = 2 * r + y
    me = s * nr + r
    unsent = []

    def place(a, b):
        return {"seq": a, "rep": b}

    def at(plane, j):
        return place(2 * plane + j % 2, j // 2)

    def send(src, dst, ssem, rsem, where):
        pltpu.make_async_remote_copy(
            src_ref=src, dst_ref=dst, send_sem=ssem, recv_sem=rsem,
            device_id=where, device_id_type=pl.DeviceIdType.MESH,
        ).start()

    def local(src, dst, rsem):
        pltpu.make_async_copy(src, dst, rsem).start()

    def landed(dst, sem):
        pltpu.make_async_copy(dst, dst, sem).wait()

    def send_if(allowed, src, dst, ssem, rsem, where):
        @pl.when(allowed)
        def _():
            send(src, dst, ssem, rsem, where)

        unsent.append((allowed, src, ssem))

    def send_or_local(src, dst, ssem, rsem, where, here):
        send_if(jnp.logical_not(here), src, dst, ssem, rsem, where)

        @pl.when(here)
        def _():
            local(src, dst, rsem)

    def rows(ref, block, count):
        return ref.at[pl.ds(pl.multiple_of(block * count, count), count), :]

    barrier = pltpu.get_barrier_semaphore()

    def greet(d, _):
        @pl.when(d != me)
        def _():
            pl.semaphore_signal(
                barrier, inc=1, device_id=place(d // nr, d % nr), device_id_type=pl.DeviceIdType.MESH
            )

        return 0

    lax.fori_loop(0, ns * nr, greet, 0)
    for j in range(nh):
        pay_src[j, :, :hb] = states[:, j * hb : (j + 1) * hb].astype(BF16)
        pay_src[j, :, hb:] = upstream[:, j * hb : (j + 1) * hb]
        tail_src[j, 0:8, :] = states[T - 8 : T, j * hb : (j + 1) * hb]
        tail_src[j, 8:16, :] = jnp.broadcast_to(ids[0:1, T - 1 : T].astype(F32), (8, hb))
    ids_src[...] = jnp.broadcast_to(ids[...].astype(F32), ids_src.shape)

    pl.semaphore_wait(barrier, ns * nr - 1)

    steps = sorted(range(nz), key=lambda step: -min(step, nz - step))
    for step in steps:
        plane = (z + step) % nz
        for i in range(GATES):
            b = GATES * s + i
            g, j = b // nh, b % nh
            dst = w_all.at[
                pl.ds(pl.multiple_of(g * hb, hb), hb), pl.ds(pl.multiple_of(r * cw, cw), cw)
            ]
            here = jnp.logical_and(step == 0, j == k)
            send_or_local(
                weight.at[i * hb : (i + 1) * hb, :], dst, w_s.at[i * nz + step],
                w_r.at[g * nr + r], at(plane, j), here,
            )
    partner = place(s, r + 1 - 2 * c)
    local(feats, rows(x_all, k, T), x_s0)

    def share(step, src, dx, dy):
        x0, y0 = (x + dx) % nx, (y + dy) % 2
        slot = 2 * (2 * x0 + c) + y0
        dst = rows(x_all, slot, T)
        src = dst if src is None else src
        if dy == 0 or dx == 0:
            for other in range(1, nx):
                if dx == 0:
                    allowed = True if dy == 0 else c == 0
                    send_if(
                        allowed, src, dst, x_sx.at[step * nx + other], x_r.at[slot],
                        place(s, 2 * ((x + other) % nx) + c),
                    )
            if dy == 0:
                allowed = True if dx == 0 else c == 1
                send_if(allowed, src, dst, x_sy.at[step], x_r.at[slot], place(2 * z + 1 - y, r))
        send_if(True, src, dst, x_sd.at[step], x_r.at[slot], partner)

    share(0, feats, 0, 0)

    for j in range(nh):
        send_or_local(ids_src, ids_all.at[k], i_s.at[j], i_r.at[k], at(z, j), k == j)
        send_or_local(pay_src.at[j], pay.at[k], p_s.at[j], p_r.at[k], at(z, j), k == j)
        send_if(
            jnp.logical_and(y == 1, z < nz - 1), tail_src.at[j], tail_in.at[r], e_s.at[j], e_r.at[r],
            at(z + 1, j),
        )

    hops = [(dx, dy) for dx in range(nx) for dy in range(2)]
    hops.sort(key=lambda hop: (hop[0] > 0) + hop[1])
    for step, (dx, dy) in enumerate(hops):
        if step > 0:
            slot = 2 * (2 * ((x + dx) % nx) + c) + (y + dy) % 2
            landed(rows(x_all, slot, T), x_r.at[slot])
            share(step, None, dx, dy)

    stride = T + 8
    for m in range(nh):
        base = m * stride + 8
        landed(ids_all.at[m], i_r.at[m])
        landed(pay.at[m], p_r.at[m])
        prev[base : base + T, :] = pay[m, :, :hb].astype(F32)
        up[m * T : (m + 1) * T, :] = pay[m, :, hb:].astype(F32)
        ids_col[base : base + T, :] = jnp.broadcast_to(ids_all[m, 0:1, :], (hb, T)).T
        if m % 2:
            before = base - stride + T
            prev[base - 8 : base, :] = prev[before - 8 : before, :]
            ids_col[base - 8 : base, :] = ids_col[before - 8 : before, :]
        else:

            @pl.when(z > 0)
            def _():
                landed(tail_in.at[m // 2], e_r.at[m // 2])
                prev[base - 8 : base, :] = tail_in[m // 2, 0:8, :]
                ids_col[base - 8 : base, :] = tail_in[m // 2, 8:16, :]

            @pl.when(z == 0)
            def _():
                prev[base - 8 : base, :] = jnp.zeros((8, hb), F32)
                ids_col[base - 8 : base, :] = jnp.full((8, hb), -1.0, F32)

    for g in range(GATES):
        for col in range(nr):
            landed(
                w_all.at[g * hb : (g + 1) * hb, col * cw : (col + 1) * cw], w_r.at[g * nr + col]
            )
    landed(rows(x_all, k, T), x_s0)
    for x0 in range(nx):
        for y0 in range(2):
            slot = 2 * (2 * x0 + 1 - c) + y0
            landed(rows(x_all, slot, T), x_r.at[slot])

    group = pl.ds(pl.multiple_of(k * hb, hb), hb)
    rz, rr, rc = (recur[i : i + 1, group] for i in range(GATES))
    bz, br, bc = (bias[i : i + 1, group] for i in range(GATES))
    pre_all[...] = lax.dot_general(
        x_all[...], w_all[...], (((1,), (1,)), ((), ())), preferred_element_type=F32
    )
    for m in range(nh):
        span = slice(m * T, (m + 1) * T)
        base = m * stride + 8
        pre = pre_all[span, :]
        same = jnp.where(
            ids_col[base : base + T, :] == ids_col[base - 1 : base - 1 + T, :], 1.0, 0.0
        )
        prior = prev[base - 1 : base - 1 + T, :] * same
        gz = jax.nn.sigmoid(pre[:, :hb] + rz * prior + bz)
        gr = jax.nn.sigmoid(pre[:, hb : 2 * hb] + rr * prior + br)
        rp = gr * prior
        gc = jnp.tanh(pre[:, 2 * hb :] + rc * rp + bc)
        az = (gc - prior) * gz * (1.0 - gz)
        ac = gz * (1.0 - gc * gc)
        slope = rp * (1.0 - gr)
        acr = ac * rc
        co_z[span, :] = az
        co_c[span, :] = ac
        co_r[span, :] = acr * slope
        rprior[span, :] = rp
        prior_all[span, :] = prior
        jac[span, :] = same * (1.0 - gz + az * rz + acr * (gr + slope * rr))

    def back(i, state):
        a, b = state
        t = T - 1 - i
        f = jac[pl.ds(t, nh, stride=T), :]
        b = b + up[pl.ds(t, nh, stride=T), :]
        scan_a[t] = a
        scan_b[t] = b
        return f * a, f * b

    a, b = lax.fori_loop(0, T, back, (jnp.ones((nh, hb), F32), jnp.zeros((nh, hb), F32)), unroll=8)
    seg_out[...] = jnp.zeros(seg_out.shape, F32)
    for o in range(nr):
        first, second = slice(2 * o, 2 * o + 1), slice(2 * o + 1, 2 * o + 2)
        seg_out[0, o : o + 1, :] = a[first, :] * a[second, :]
        seg_out[1, o : o + 1, :] = b[first, :] + a[first, :] * b[second, :]
    for plane in range(nz - 1):
        send_if(plane < z, seg_out, seg_in.at[z], c_s.at[plane], c_r.at[z], at(plane, k))
    carry[...] = jnp.zeros(carry.shape, F32)
    for plane in reversed(range(1, nz)):

        @pl.when(plane > z)
        def _():
            landed(seg_in.at[plane], c_r.at[plane])
            carry[0:nr, :] = seg_in[plane, 1, 0:nr, :] + seg_in[plane, 0, 0:nr, :] * carry[0:nr, :]

    into = carry[0:nr, :]
    carry_rows = []
    for o in range(nr):
        later = into[o : o + 1, :]
        second = slice(2 * o + 1, 2 * o + 2)
        carry_rows += [b[second, :] + a[second, :] * later, later]
    carried = jnp.concatenate(carry_rows, 0)

    def finish(t, _):
        lam[pl.ds(t, nh, stride=T), :] = scan_b[t] + scan_a[t] * carried
        return 0

    lax.fori_loop(0, T, finish, 0, unroll=8)

    sums = [jnp.zeros((1, hb), F32) for _ in range(6)]
    for m in range(nh):
        span = slice(m * T, (m + 1) * T)
        prior = prior_all[span, :]
        adj = lam[span, :]
        grad_z = adj * co_z[span, :]
        grad_r = adj * co_r[span, :]
        grad_c = adj * co_c[span, :]
        grads[span, :hb] = grad_z.astype(BF16)
        grads[span, hb : 2 * hb] = grad_r.astype(BF16)
        grads[span, 2 * hb :] = grad_c.astype(BF16)
        terms = (grad_z, grad_r, grad_c, grad_z * prior, grad_r * prior, grad_c * rprior[span, :])
        sums = [total + jnp.sum(term, 0, keepdims=True) for total, term in zip(sums, terms)]
    for i in range(6):
        st_out[i : i + 1, :] = sums[i]
    st_out[6:8, :] = jnp.zeros((2, hb), F32)

    slot = k * nz + z
    st_in[slot] = st_out[...]

    def tell(d, _):
        @pl.when(d != me)
        def _():
            send(st_out, st_in.at[slot], t_s.at[d], t_r.at[slot], place(d // nr, d % nr))

        return 0

    lax.fori_loop(0, ns * nr, tell, 0)

    wide = lax.dot_general(
        grads[...], x_all[...], (((0,), (0,)), ((), ())), preferred_element_type=F32
    )
    for g in range(GATES):
        wg_out[g] = wide[g * hb : (g + 1) * hb, :].astype(BF16)
    for n in range(GATES):
        g = jnp.where(z < nz // 2, GATES - 1 - n, n)
        b = g * nh + k
        owner, i = b // GATES, b % GATES
        for col in range(nr):
            here = jnp.logical_and(owner == s, r == col)
            send_or_local(
                wg_out.at[g, :, col * cw : (col + 1) * cw], wg_in.at[z * GATES + i],
                g_s.at[n * nr + col], g_r.at[z * GATES + i], place(owner, col), here,
            )

    chips = [(x0, y0) for x0 in range(nx) for y0 in range(2)]
    for x0 in range(nx):
        wide = jnp.dot(
            rows(grads, 2 * x0 + 1 - c, 2 * T)[...], w_all[...], preferred_element_type=F32
        )
        for n in (2 * x0, 2 * x0 + 1):
            part_out[n] = wide[(n % 2) * T : (n % 2 + 1) * T, :].astype(BF16)
            send_if(True, part_out.at[n], part_in.at[n], d_s.at[n], d_r.at[n], partner)
    for x0 in range(nx):
        wide = jnp.dot(
            rows(grads, 2 * x0 + c, 2 * T)[...], w_all[...], preferred_element_type=F32
        )
        for n in (2 * x0, 2 * x0 + 1):
            part_keep[n] = wide[(n % 2) * T : (n % 2 + 1) * T, :]
    chip = 2 * x + y
    for n, (x0, y0) in enumerate(chips):
        landed(part_in.at[n], d_r.at[n])
        fin_out[n] = (part_keep[n] + part_in[n].astype(F32)).astype(BF16)
        send_or_local(
            fin_out.at[n], fin_in.at[chip], f_s.at[n], f_r.at[chip],
            place(2 * z + y0, 2 * x0 + c), chip == n,
        )

    scale = 1.0 / math.sqrt(ns * nr * T)

    def heard(d, _):
        @pl.when(d != slot)
        def _():
            landed(st_in.at[d], t_r.at[d])

        return 0

    lax.fori_loop(0, ns * nr, heard, 0)
    for j in range(nh):
        total = st_in[j * nz]
        for other in range(1, nz):
            total = total + st_in[j * nz + other]
        out_p[:, j * hb : (j + 1) * hb] = total[:6] * scale

    total = None
    for n in range(len(chips)):
        landed(fin_in.at[n], f_r.at[n])
        term = fin_in[n].astype(F32)
        total = term if total is None else total + term
    out_in[...] = total.astype(BF16)

    for i in range(GATES):
        total = None
        for other in range(nz):
            landed(wg_in.at[other * GATES + i], g_r.at[other * GATES + i])
            term = wg_in[other * GATES + i].astype(F32)
            total = term if total is None else total + term
        out_w[i * hb : (i + 1) * hb, :] = total * scale

    def told(d, _):
        @pl.when(d != me)
        def _():
            landed(st_out, t_s.at[d])

        return 0

    lax.fori_loop(0, ns * nr, told, 0)
    for sent, src, sem in unsent:
        if sent is True:
            landed(src, sem)
        else:

            @pl.when(sent)
            def _():
                landed(src, sem)


def by_hidden(ns, nr, inputs, weight_t, states, doc_ids, recur, bias, out_grad):
    T, DI = inputs.shape[1:]
    H = states.shape[2]
    nh, nz, nx = 2 * nr, ns // 2, nr // 2
    hb, cw = H // nh, DI // nr
    L = nh * T
    vm = pltpu.VMEM
    scratch = [
        vm((nh, T, 2 * hb), BF16),
        vm((nh, T, 2 * hb), BF16),
        vm((8, T), F32),
        vm((nh, 8, T), F32),
        vm((nh, 16, hb), F32),
        vm((nr, 16, hb), F32),
        vm((L, DI), BF16),
        vm((GATES * hb, DI), BF16),
        vm((L + 8 * nh, hb), F32),
        vm((L + 8 * nh, hb), F32),
        vm((L, hb), F32),
        vm((L, hb), F32),
        vm((L, hb), F32),
        vm((L, hb), F32),
        vm((L, hb), F32),
        vm((L, hb), F32),
        vm((L, hb), F32),
        vm((T, nh, hb), F32),
        vm((T, nh, hb), F32),
        vm((nh, hb), F32),
        vm((2, 8, hb), F32),
        vm((nz, 2, 8, hb), F32),
        vm((L, hb), F32),
        vm((L, GATES * hb), BF16),
        vm((nr, T, DI), BF16),
        vm((nr, T, DI), BF16),
        vm((nr, T, DI), F32),
        vm((nr, T, DI), BF16),
        vm((nr, T, DI), BF16),
        vm((GATES, hb, DI), BF16),
        vm((nz * GATES, hb, cw), BF16),
        vm((8, hb), F32),
        vm((ns * nr, 8, hb), F32),
        vm((L, GATES * hb), F32),
    ]
    dma = pltpu.SemaphoreType.DMA
    counts = [
        None, nr * nx, nr, nr, nh, GATES * nz, GATES * nr, nh, nh, nh, nh, nh, nr, nz, nz, nr, nr, nr, nr,
        GATES * nr, GATES * nz, ns * nr, ns * nr,
    ]
    sems = [dma if n is None else dma((n,)) for n in counts]
    whole = pl.BlockSpec(memory_space=pltpu.VMEM)
    out_in, out_w, out_p = pl.pallas_call(
        functools.partial(kernel, ns, nr),
        out_shape=(
            jax.ShapeDtypeStruct((T, DI), BF16),
            jax.ShapeDtypeStruct(weight_t.shape, F32),
            jax.ShapeDtypeStruct((6, H), F32),
        ),
        in_specs=[whole] * 7,
        out_specs=(whole,) * 3,
        scratch_shapes=scratch + sems,
        compiler_params=pltpu.CompilerParams(
            collective_id=0, has_side_effects=True, vmem_limit_bytes=56 * 1024 * 1024
        ),
    )(inputs[0], weight_t, states[0], doc_ids, recur, bias, out_grad[0])
    return out_in[None], out_w, out_p


def fits(ns, nr, inputs, weight_t, states):
    parts, L, DI = inputs.shape
    H = states.shape[2]
    return (
        parts == nr
        and ns == 2 * nr
        and ns % 8 == 0
        and ns == 8
        and H % (ns * 128) == 0
        and DI % (nr * 128) == 0
        and L % (ns * 128) == 0
        and L * DI <= 1 << 21
    )


def solution(mesh):
    ns, nr = mesh.shape["seq"], mesh.shape["rep"]
    placed = (
        P("rep", "seq", None),
        P("seq", "rep"),
        P("rep", "seq", None),
        P("rep", "seq"),
        P(),
        P(),
        P("rep", "seq", None),
    )

    def run(inputs, weight_t, states, doc_ids, recur, bias, out_grad):
        kernelized = fits(ns, nr, inputs, weight_t, states)
        body = functools.partial(by_hidden, ns, nr) if kernelized else by_tokens
        return jax.shard_map(
            body,
            mesh=mesh,
            in_specs=placed,
            out_specs=(P("rep", "seq", None), P("seq", "rep"), P()),
            check_vma=False,
        )(inputs, weight_t, states, doc_ids, recur, bias, out_grad)

    return run
```
